32 devices in a mesh: rows: 4 (over x, core), cols: 8 (over z, y).
Axes of the slice: x: 2, y: 2, z: 4, core: 2. Of those that a mesh axis runs over, the one named last changes fastest.
Arguments:
- samples: bfloat16 [2048, 65536], P('rows', 'cols'), may hold values from -0.0234375 to 0.0234375
- labels: int32 [2048], P('rows'), may hold values 0 or 1
- weights: float32 [65536], P('cols'), may hold values from -7 to 7, as said below
- hist_s: float32 [16, 65536], P(None, 'cols'), may hold values from -60 to 60
- hist_y: float32 [16, 65536], P(None, 'cols'), may hold values from -480 to 480, as said below
- counter: int32 [1], replicated, may hold values from 0 to 4095
Outputs:
- new_weights: float32 [65536], P('cols')
- gradient: float32 [65536], P('cols')
The draws below stay inside these ranges and needn't reach their ends.
Inputs may be any that keep to these rules, and one draw needn't show every extreme that they name: weights share a common direction with the rows of hist_s. Each entry of hist_y[j] is a positive multiple of the same entry of hist_s[j], so s_j . y_j > 0.
All inputs are finite; a program needn't handle non-finite values. No bound on the sum of `labels` on one device may be relied on, other than what follows from the above.
Results may differ from the reference program's by a relative error of at most 0.0013.
Values sent between devices are 32-bit elements; how exact they have to be, the bound alone decides.
No kernel may reach another device: no remote copies, remote signals or barrier semaphores. Data moves between devices by JAX's collectives and lax.ppermute only.
A program may use at most 64 MiB of HBM per device.

```python
import math
import jax
import jax.numpy as jnp
from jax import lax

FEAT = 65536
HIST = 16
SAMPLES = 2048


def common_base(key):
    return jax.random.truncated_normal(jax.random.fold_in(key, 101), -4.0, 4.0, (FEAT,), jnp.float32)


def draw_weights(key, part):
    base = common_base(key)
    noise = jax.random.truncated_normal(jax.random.fold_in(key, 103), -4.0, 4.0, (FEAT,), jnp.float32)
    return base + 0.5 * noise


def draw_hist_s(key, part):
    base = common_base(key)
    mixing = jax.random.uniform(jax.random.fold_in(key, 107), (HIST, 1), jnp.float32, -1.0, 1.0)
    noise = jax.random.truncated_normal(jax.random.fold_in(key, 109), -4.0, 4.0, (HIST, FEAT), jnp.float32)
    field = mixing * base[None, :] + 0.5 * noise
    return field


def draw_hist_y(key, part):
    field = draw_hist_s(key, part)
    factor = jnp.exp(jax.random.uniform(jax.random.fold_in(key, 127), (HIST, FEAT), jnp.float32, math.log(0.5), math.log(4.0)))
    return factor * field


def touch_ends(array, key, least, top_value):
    longest = array.shape.index(max(array.shape))
    spots = []
    for shift in (0, 1):
        where = [jax.random.randint(jax.random.fold_in(key, axis), (), 0, length) for axis, length in enumerate(array.shape)]
        where[longest] = (where[longest] + shift) % array.shape[longest]
        spots.append(tuple(where))
    return array.at[spots[0]].set(least).at[spots[1]].set(top_value)


def shard_levels(key, dims, shards, low, top_value):
    factor_of, own = 1.0, jax.random.fold_in(key, 6)
    for position, parts in shards:
        steps = jnp.exp(jax.random.uniform(jax.random.fold_in(own, position), (parts,), jnp.float32, low / len(shards), top_value / len(shards)))
        factor_of = factor_of * jnp.repeat(steps, dims[position] // parts).reshape([-1 if axis == position else 1 for axis in range(len(dims))])
    return factor_of


def scatter_about(rng, extent, scale, limit, cuts=(), held_as=jnp.bfloat16):
    factor_of = shard_levels(rng, extent, cuts, -0.22, 0.18) if cuts else 1.0
    drawn = jax.random.normal(rng, extent, jnp.float32) * scale * factor_of
    return jnp.minimum(jnp.maximum(drawn, -limit), limit).astype(held_as)


def setup_inputs(seed: int = 0) -> dict:
    key_list = jax.random.split(jax.random.key(seed), 7)
    samples = scatter_about(key_list[0], (SAMPLES, FEAT), FEAT ** -0.5, 0.0234375, ((0, 4), (1, 8)))
    labels = touch_ends((jax.random.randint(key_list[1], (SAMPLES,), 0, 2) < 1).astype(jnp.int32), jax.random.fold_in(key_list[1], 1), 0, 1)
    weights = draw_weights(jax.random.fold_in(key_list[6], 71), 0)
    hist_s = draw_hist_s(jax.random.fold_in(key_list[6], 71), 0)
    hist_y = draw_hist_y(jax.random.fold_in(key_list[6], 71), 0)
    counter = jax.random.randint(key_list[5], (1,), 0, 4096).astype(jnp.int32)
    return {"samples": samples, "labels": labels, "weights": weights, "hist_s": hist_s, "hist_y": hist_y, "counter": counter}


penalty = 4.0
step_length = 0.5


def pick(table, slot):
    return lax.dynamic_index_in_dim(table, slot, 0, keepdims=False)


def reference(samples, labels, weights, hist_s, hist_y, counter):
    margin = jnp.dot(samples, weights.astype(jnp.bfloat16), preferred_element_type=jnp.float32)
    resid = (jax.nn.sigmoid(margin) - labels.astype(jnp.float32)).astype(jnp.bfloat16)
    total = jnp.dot(resid, samples, preferred_element_type=jnp.float32)
    gradient = weights + penalty * total
    newest = (counter[0] % HIST).astype(jnp.int32)
    curv = jnp.sum(hist_s * hist_y, axis=1)
    rho = 1.0 / curv
    y_new = pick(hist_y, newest)
    gamma = pick(curv, newest) / jnp.sum(y_new * y_new)
    query = gradient
    coefs = []
    slots = []
    for step in range(HIST):
        slot = ((newest - step) % HIST).astype(jnp.int32)
        slots.append(slot)
        coef = pick(rho, slot) * jnp.sum(pick(hist_s, slot) * query)
        coefs.append(coef)
        query = query - coef * pick(hist_y, slot)
    result = gamma * query
    for step in reversed(range(HIST)):
        slot = slots[step]
        beta = pick(rho, slot) * jnp.sum(pick(hist_y, slot) * result)
        result = result + (coefs[step] - beta) * pick(hist_s, slot)
    return weights - step_length * result, gradient
```

```python
import jax
import jax.numpy as jnp
from jax import lax
from jax.experimental import pallas as pl
from jax.experimental.pallas import tpu as pltpu
from jax.sharding import PartitionSpec as P

HIST = 16
LANES = 128
TAIL = 8

penalty = 4.0
step_length = 0.5
highest = lax.Precision.HIGHEST

ANY = pl.BlockSpec(memory_space=pl.ANY)
VM = pl.BlockSpec(memory_space=pltpu.VMEM)
SM = pl.BlockSpec(memory_space=pltpu.SMEM)
SMALL_GRANT = pltpu.CompilerParams(vmem_limit_bytes=16 << 20)


def pieces(values):
    out = []
    for _ in range(3):
        part = values.astype(jnp.bfloat16)
        out.append(part)
        values = values - part.astype(jnp.float32)
    return out


def contract_last(left, right):
    dims = (((1,), (1,)), ((), ()))
    return lax.dot_general(left, right, dims, preferred_element_type=jnp.float32)


def first_kernel(chunks, x_hbm, w_hbm, s_hbm, y_hbm, x_out, w_out, s_out, y_out, pay, z_buf, small_sem, x_sem):
    rows, width = x_out.shape
    step = width // chunks
    smalls = [
        pltpu.make_async_copy(src, dst, small_sem.at[k])
        for k, (src, dst) in enumerate(((w_hbm, w_out), (s_hbm, s_out), (y_hbm, y_out)))
    ]
    bigs = [
        pltpu.make_async_copy(
            x_hbm.at[:, pl.ds(c * step, step)], x_out.at[:, pl.ds(c * step, step)], x_sem.at[c]
        )
        for c in range(chunks)
    ]
    for copy in smalls + bigs:
        copy.start()
    for copy in smalls:
        copy.wait()
    for c in range(chunks):
        cut = pl.ds(c * step, step)
        both = jnp.concatenate([s_out[:, cut], y_out[:, cut]], axis=0)
        for k, part in enumerate(pieces(both)):
            z_buf[2 * HIST * k : 2 * HIST * (k + 1), cut] = part
        w_parts = pieces(w_out[:, cut])
        place = lax.broadcasted_iota(jnp.int32, (HIST, step), 0)
        w_rows = jnp.zeros((HIST, step), jnp.float32)
        for k, part in enumerate(w_parts):
            w_rows = jnp.where(place == k, part.astype(jnp.float32), w_rows)
        z_buf[6 * HIST :, cut] = w_rows.astype(jnp.bfloat16)
    with_x = jnp.zeros((7 * HIST, rows), jnp.float32)
    with_z = jnp.zeros((7 * HIST, 7 * HIST), jnp.float32)
    for c in range(chunks):
        cut = pl.ds(c * step, step)
        z_part = z_buf[:, cut]
        with_z = with_z + contract_last(z_part, z_part)
    for c in range(chunks):
        cut = pl.ds(c * step, step)
        z_part = z_buf[:, cut]
        bigs[c].wait()
        with_x = with_x + contract_last(z_part, x_out[:, cut])
    both = 2 * HIST
    pay[:both, :] = with_x[:both] + (with_x[both : 2 * both] + with_x[2 * both : 3 * both])
    pay[both:, :] = jnp.zeros((TAIL, rows), jnp.float32)
    pay[both : both + 1, :] = with_x[3 * both : 3 * both + 1]
    gram = with_z[:both] + (with_z[both : 2 * both] + with_z[2 * both : 3 * both])
    of_y = gram[:, HIST:both] + (gram[:, 3 * HIST : 4 * HIST] + gram[:, 5 * HIST : 6 * HIST])
    at = 6 * HIST
    of_w = gram[:, at : at + 1] + (gram[:, at + 1 : at + 2] + gram[:, at + 2 : at + 3])
    wide = jnp.concatenate([of_y[:HIST], of_y[HIST:], of_w[:HIST], of_w[HIST:]], axis=1)
    for k in range(4):
        pay[both + 4 : both + 8, LANES * k : LANES * k + both + 2] = wide[4 * k : 4 * k + 4]


def second_kernel(chunks, x_ref, own, got, label_ref, pay, gram):
    both = 2 * HIST
    rows, width = x_ref.shape
    step = width // chunks
    tail = own[both:, :] + got[both:, :]
    gram[...] = tail
    margin = tail[0:1, :]
    resid = (jax.nn.sigmoid(margin) - label_ref[...].astype(jnp.float32)).astype(jnp.bfloat16)
    for c in range(chunks):
        cut = pl.ds(c * step, step)
        pay[:, cut] = jnp.dot(resid, x_ref[:, cut], preferred_element_type=jnp.float32)
    cross = (own[:both, :] + got[:both, :]) * resid.astype(jnp.float32)
    column = jnp.sum(cross, axis=1, keepdims=True)
    row_at = lax.broadcasted_iota(jnp.int32, (both, LANES), 0)
    lane_at = lax.broadcasted_iota(jnp.int32, (both, LANES), 1)
    pay[:, width:] = jnp.sum(jnp.where(row_at == lane_at, column, 0.0), axis=0, keepdims=True)


def to_column(row, count):
    row_at = lax.broadcasted_iota(jnp.int32, (count, count), 0)
    lane_at = lax.broadcasted_iota(jnp.int32, (count, count), 1)
    return jnp.sum(jnp.where(row_at == lane_at, row, 0.0), axis=1, keepdims=True)


def solve_kernel(counter, gram, out):
    newest = lax.rem(counter[0], HIST)
    wide = jnp.concatenate(
        [gram[4:8, LANES * k : LANES * (k + 1)] for k in range(4)], axis=0
    )
    sy = wide[:, :HIST]
    yy = wide[:, HIST : 2 * HIST]
    row_at = lax.broadcasted_iota(jnp.int32, (HIST, HIST), 0)
    lane_at = lax.broadcasted_iota(jnp.int32, (HIST, HIST), 1)
    row_age = lax.rem(newest - row_at + HIST, HIST)
    lane_age = lax.rem(newest - lane_at + HIST, HIST)
    eye = row_at == lane_at
    diag_col = jnp.sum(jnp.where(eye, sy, 0.0), axis=1, keepdims=True)
    rho_col = 1.0 / diag_col
    strict = jnp.where(lane_age < row_age, sy, 0.0) * rho_col
    rest = jnp.where(eye, rho_col, 0.0)
    for age in range(HIST - 1):
        column = jnp.sum(jnp.where(lane_age == age, strict, 0.0), axis=1, keepdims=True)
        row = jnp.sum(jnp.where(row_age == age, rest, 0.0), axis=0, keepdims=True)
        rest = rest - column * row
    at_new = jnp.logical_and(row_at == newest, lane_at == newest)
    top = jnp.sum(jnp.sum(jnp.where(at_new, sy, 0.0), axis=1, keepdims=True), axis=0, keepdims=True)
    low = jnp.sum(jnp.sum(jnp.where(at_new, yy, 0.0), axis=1, keepdims=True), axis=0, keepdims=True)
    gamma = top / low
    middle = jnp.where(eye, diag_col, 0.0) + gamma * yy
    right = jnp.dot(middle, rest, precision=highest, preferred_element_type=jnp.float32)
    flip = (((0,), (0,)), ((), ()))
    corner = lax.dot_general(rest, right, flip, precision=highest, preferred_element_type=jnp.float32)
    turned = lax.dot_general(
        rest, jnp.where(eye, 1.0, 0.0), flip, precision=highest, preferred_element_type=jnp.float32
    )
    out[...] = jnp.zeros(out.shape, jnp.float32)
    out[0:HIST, 0:HIST] = corner
    out[0:HIST, HIST : 2 * HIST] = -gamma * turned
    out[HIST : 2 * HIST, 0:HIST] = -gamma * rest
    ones = jnp.ones((1, LANES), jnp.float32)
    out[2 * HIST : 2 * HIST + 1, :] = gamma * ones
    w_col = jnp.concatenate([wide[:, 2 * HIST : 2 * HIST + 1], wide[:, 2 * HIST + 1 : 2 * HIST + 2]], axis=0)
    big_row = lax.broadcasted_iota(jnp.int32, (2 * HIST, LANES), 0)
    big_lane = lax.broadcasted_iota(jnp.int32, (2 * HIST, LANES), 1)
    out[2 * HIST + 1 : 2 * HIST + 2, :] = jnp.sum(
        jnp.where(big_row == big_lane, w_col, 0.0), axis=0, keepdims=True
    )


def last_kernel(chunks, count, *refs):
    parts = refs[:count]
    coef_ref, w_ref, s_ref, y_ref, new_ref, grad_ref = refs[count:]
    both = 2 * HIST
    width = w_ref.shape[1]
    step = width // chunks

    def summed(cut):
        level = [p[:, cut] for p in parts]
        while len(level) > 1:
            level = [level[k] + level[k + 1] for k in range(0, len(level), 2)]
        return level[0]

    dots = coef_ref[both + 1 : both + 2, :] + penalty * summed(pl.ds(width, LANES))
    gamma = coef_ref[both : both + 1, 0:1]
    coef = jnp.sum(coef_ref[:both, :] * dots, axis=1, keepdims=True)
    for c in range(chunks):
        cut = pl.ds(c * step, step)
        weights = w_ref[:, cut]
        gradient = weights + penalty * summed(cut)
        grad_ref[:, cut] = gradient
        mixed = coef[:HIST] * s_ref[:, cut] + coef[HIST:] * y_ref[:, cut]
        turn = gamma * gradient + jnp.sum(mixed, axis=0, keepdims=True)
        new_ref[:, cut] = weights - step_length * turn


def hop(values, axis, bit):
    size = lax.axis_size(axis)
    return lax.ppermute(values, axis, [(k, k ^ bit) for k in range(size)])


def body(samples, labels, weights, hist_s, hist_y, counter):
    rows, width = samples.shape
    both = 2 * HIST
    f32 = jnp.float32
    chunks = 8
    w_row = weights.reshape(1, width)
    x_in, w_in, s_in, y_in, pay = pl.pallas_call(
        lambda *refs: first_kernel(chunks, *refs),
        in_specs=[ANY] * 4,
        out_specs=[VM] * 5,
        out_shape=[
            pltpu.VMEM((rows, width), jnp.bfloat16),
            pltpu.VMEM((1, width), f32),
            pltpu.VMEM((HIST, width), f32),
            pltpu.VMEM((HIST, width), f32),
            pltpu.VMEM((both + TAIL, rows), f32),
        ],
        scratch_shapes=[
            pltpu.VMEM((7 * HIST, width), jnp.bfloat16),
            pltpu.SemaphoreType.DMA((3,)),
            pltpu.SemaphoreType.DMA((chunks,)),
        ],
        compiler_params=SMALL_GRANT,
        name="load_and_project",
    )(samples, w_row, hist_s, hist_y)

    bit = 1
    cols = lax.axis_size("cols")
    while 2 * bit < cols:
        pay = pay + hop(pay, "cols", bit)
        bit *= 2
    got = hop(pay, "cols", bit) if cols > 1 else jnp.zeros_like(pay)

    part, gram = pl.pallas_call(
        lambda *refs: second_kernel(chunks, *refs),
        in_specs=[VM] * 4,
        out_specs=[VM] * 2,
        out_shape=[pltpu.VMEM((1, width + LANES), f32), pltpu.VMEM((TAIL, rows), f32)],
        compiler_params=SMALL_GRANT,
        name="residual_and_gradient",
    )(x_in, pay, got, labels.reshape(1, rows))

    coefs = pl.pallas_call(
        solve_kernel,
        in_specs=[SM, VM],
        out_specs=VM,
        out_shape=pltpu.VMEM((both + TAIL, LANES), f32),
        compiler_params=SMALL_GRANT,
        name="solve_history",
    )(counter, gram)

    size = lax.axis_size("rows")
    bit = size // 2
    while bit > 2:
        part = part + hop(part, "rows", bit)
        bit //= 2
    parts = [part] + [hop(part, "rows", k) for k in range(1, min(size, 4))]

    new_w, grad = pl.pallas_call(
        lambda *refs: last_kernel(chunks, len(parts), *refs),
        in_specs=[VM] * (len(parts) + 4),
        out_specs=[VM] * 2,
        out_shape=[jax.ShapeDtypeStruct((1, width), f32)] * 2,
        compiler_params=SMALL_GRANT,
        name="direction_and_update",
    )(*parts, coefs, w_in, s_in, y_in)
    return new_w.reshape(width), grad.reshape(width)


def solution(mesh):
    in_specs = (P("rows", "cols"), P("rows"), P("cols"), P(None, "cols"), P(None, "cols"), P())
    out_specs = (P("cols"), P("cols"))
    return jax.shard_map(body, mesh=mesh, in_specs=in_specs, out_specs=out_specs, check_vma=False)
```

```python
import jax
import jax.numpy as jnp
from jax import lax
from jax.experimental import pallas as pl
from jax.experimental.pallas import tpu as pltpu
from jax.sharding import PartitionSpec as P

HIST = 16
LANES = 128
TAIL = 8

penalty = 4.0
step_length = 0.5
highest = lax.Precision.HIGHEST

HBM = pl.BlockSpec(memory_space=pltpu.HBM)
VM = pl.BlockSpec(memory_space=pltpu.VMEM)
SM = pl.BlockSpec(memory_space=pltpu.SMEM)
SMALL_GRANT = pltpu.CompilerParams(vmem_limit_bytes=16 << 20)


def pieces(values):
    out = []
    for _ in range(3):
        part = values.astype(jnp.bfloat16)
        out.append(part)
        values = values - part.astype(jnp.float32)
    return out


def contract_last(left, right):
    dims = (((1,), (1,)), ((), ()))
    return lax.dot_general(left, right, dims, preferred_element_type=jnp.float32)


def first_kernel(blocks, place_ref, x_hbm, w_hbm, s_hbm, y_hbm, pay, x_out, w_out, s_out, y_out, acc, z_buf, sem):
    rows, width = x_out.shape
    both = 2 * HIST
    step = width // sum(blocks)
    smalls = [
        pltpu.make_async_copy(src, dst, sem.at[k])
        for k, (src, dst) in enumerate(((w_hbm, w_out), (s_hbm, s_out), (y_hbm, y_out)))
    ]
    bigs = [
        pltpu.make_async_copy(
            x_hbm.at[:, pl.ds(c * step, step)], x_out.at[:, pl.ds(c * step, step)], sem.at[3 + c]
        )
        for c in range(sum(blocks))
    ]
    for copy in smalls + bigs:
        copy.start()
    live = place_ref[0] >= 0
    for copy in smalls:
        copy.wait()

    @pl.when(live)
    def _():
        part_width = width // 8
        for c in range(8):
            cut = pl.ds(c * part_width, part_width)
            hist = jnp.concatenate([s_out[:, cut], y_out[:, cut]], axis=0)
            for k, part in enumerate(pieces(hist)):
                z_buf[both * k : both * (k + 1), cut] = part
            place = lax.broadcasted_iota(jnp.int32, (both, part_width), 0)
            w_rows = jnp.zeros((both, part_width), jnp.float32)
            for k, part in enumerate(pieces(w_out[:, cut])):
                w_rows = jnp.where(place == k, part.astype(jnp.float32), w_rows)
            z_buf[3 * both :, cut] = w_rows.astype(jnp.bfloat16)
        acc[rows:] = contract_last(z_buf[...], z_buf[...])

    at = 0
    for n, size in enumerate(blocks):
        for c in range(at, at + size):
            bigs[c].wait()

        @pl.when(live)
        def _(n=n, size=size, at=at):
            cut = pl.ds(at * step, size * step)
            product = contract_last(x_out[:, cut], z_buf[:, cut])
            if n == 0:
                acc[:rows] = product
            else:
                acc[:rows] += product

        at += size

    @pl.when(live)
    def _():
        with_x = jnp.transpose(acc[:rows])
        pay[:both] = with_x[:both] + (with_x[both : 2 * both] + with_x[2 * both : 3 * both])
        pay[both:] = with_x[3 * both : 3 * both + TAIL]
        with_z = acc[rows:]
        gram = with_z[:both] + (with_z[both : 2 * both] + with_z[2 * both : 3 * both])
        of_y = gram[:, HIST:both] + (gram[:, 3 * HIST : 4 * HIST] + gram[:, 5 * HIST : 6 * HIST])
        at = 6 * HIST
        of_w = gram[:, at : at + 1] + (gram[:, at + 1 : at + 2] + gram[:, at + 2 : at + 3])
        wide = jnp.concatenate([of_y[:HIST], of_y[HIST:], of_w[:HIST], of_w[HIST:]], axis=1)
        for k in range(4):
            pay[both + 4 : both + 8, LANES * k : LANES * k + both + 2] = wide[4 * k : 4 * k + 4]


def second_kernel(chunks, x_ref, own, got, label_ref, pay, gram):
    both = 2 * HIST
    rows, width = x_ref.shape
    step = width // chunks
    tail = own[both:, :] + got[both:, :]
    gram[...] = tail
    margin = tail[0:1, :]
    resid = (jax.nn.sigmoid(margin) - label_ref[...].astype(jnp.float32)).astype(jnp.bfloat16)
    for c in range(chunks):
        cut = pl.ds(c * step, step)
        pay[:, cut] = jnp.dot(resid, x_ref[:, cut], preferred_element_type=jnp.float32)
    cross = (own[:both, :] + got[:both, :]) * resid.astype(jnp.float32)
    column = jnp.sum(cross, axis=1, keepdims=True)
    row_at = lax.broadcasted_iota(jnp.int32, (both, LANES), 0)
    lane_at = lax.broadcasted_iota(jnp.int32, (both, LANES), 1)
    pay[:, width:] = jnp.sum(jnp.where(row_at == lane_at, column, 0.0), axis=0, keepdims=True)


def to_column(row, count):
    row_at = lax.broadcasted_iota(jnp.int32, (count, count), 0)
    lane_at = lax.broadcasted_iota(jnp.int32, (count, count), 1)
    return jnp.sum(jnp.where(row_at == lane_at, row, 0.0), axis=1, keepdims=True)


def solve_kernel(counter, gram, out):
    newest = lax.rem(counter[0], HIST)
    wide = jnp.concatenate(
        [gram[4:8, LANES * k : LANES * (k + 1)] for k in range(4)], axis=0
    )
    sy = wide[:, :HIST]
    yy = wide[:, HIST : 2 * HIST]
    row_at = lax.broadcasted_iota(jnp.int32, (HIST, HIST), 0)
    lane_at = lax.broadcasted_iota(jnp.int32, (HIST, HIST), 1)
    row_age = lax.rem(newest - row_at + HIST, HIST)
    lane_age = lax.rem(newest - lane_at + HIST, HIST)
    eye = row_at == lane_at
    diag_col = jnp.sum(jnp.where(eye, sy, 0.0), axis=1, keepdims=True)
    rho_col = 1.0 / diag_col
    strict = jnp.where(lane_age < row_age, sy, 0.0) * rho_col
    rest = jnp.where(eye, rho_col, 0.0)
    for age in range(HIST - 1):
        column = jnp.sum(jnp.where(lane_age == age, strict, 0.0), axis=1, keepdims=True)
        row = jnp.sum(jnp.where(row_age == age, rest, 0.0), axis=0, keepdims=True)
        rest = rest - column * row
    at_new = jnp.logical_and(row_at == newest, lane_at == newest)
    top = jnp.sum(jnp.sum(jnp.where(at_new, sy, 0.0), axis=1, keepdims=True), axis=0, keepdims=True)
    low = jnp.sum(jnp.sum(jnp.where(at_new, yy, 0.0), axis=1, keepdims=True), axis=0, keepdims=True)
    gamma = top / low
    middle = jnp.where(eye, diag_col, 0.0) + gamma * yy
    right = jnp.dot(middle, rest, precision=highest, preferred_element_type=jnp.float32)
    flip = (((0,), (0,)), ((), ()))
    corner = lax.dot_general(rest, right, flip, precision=highest, preferred_element_type=jnp.float32)
    turned = lax.dot_general(
        rest, jnp.where(eye, 1.0, 0.0), flip, precision=highest, preferred_element_type=jnp.float32
    )
    out[...] = jnp.zeros(out.shape, jnp.float32)
    out[0:HIST, 0:HIST] = corner
    out[0:HIST, HIST : 2 * HIST] = -gamma * turned
    out[HIST : 2 * HIST, 0:HIST] = -gamma * rest
    ones = jnp.ones((1, LANES), jnp.float32)
    out[2 * HIST : 2 * HIST + 1, :] = gamma * ones
    w_col = jnp.concatenate([wide[:, 2 * HIST : 2 * HIST + 1], wide[:, 2 * HIST + 1 : 2 * HIST + 2]], axis=0)
    big_row = lax.broadcasted_iota(jnp.int32, (2 * HIST, LANES), 0)
    big_lane = lax.broadcasted_iota(jnp.int32, (2 * HIST, LANES), 1)
    out[2 * HIST + 1 : 2 * HIST + 2, :] = jnp.sum(
        jnp.where(big_row == big_lane, w_col, 0.0), axis=0, keepdims=True
    )


def last_kernel(chunks, count, *refs):
    parts = refs[:count]
    coef_ref, w_ref, s_ref, y_ref, new_ref, grad_ref = refs[count:]
    both = 2 * HIST
    width = w_ref.shape[1]
    step = width // chunks

    def summed(cut):
        level = [p[:, cut] for p in parts]
        while len(level) > 1:
            level = [level[k] + level[k + 1] for k in range(0, len(level), 2)]
        return level[0]

    dots = coef_ref[both + 1 : both + 2, :] + penalty * summed(pl.ds(width, LANES))
    gamma = coef_ref[both : both + 1, 0:1]
    coef = jnp.sum(coef_ref[:both, :] * dots, axis=1, keepdims=True)
    for c in range(chunks):
        cut = pl.ds(c * step, step)
        weights = w_ref[:, cut]
        gradient = weights + penalty * summed(cut)
        grad_ref[:, cut] = gradient
        mixed = coef[:HIST] * s_ref[:, cut] + coef[HIST:] * y_ref[:, cut]
        turn = gamma * gradient + jnp.sum(mixed, axis=0, keepdims=True)
        new_ref[:, cut] = weights - step_length * turn


def hop(values, axis, bit):
    size = lax.axis_size(axis)
    return lax.ppermute(values, axis, [(k, k ^ bit) for k in range(size)])


def body(samples, labels, weights, hist_s, hist_y, counter):
    rows, width = samples.shape
    both = 2 * HIST
    f32 = jnp.float32
    chunks = 8
    blocks = (3, 4, 5, 4)
    w_row = weights.reshape(1, width)
    pay, x_in, w_in, s_in, y_in = pl.pallas_call(
        lambda *refs: first_kernel(blocks, *refs),
        in_specs=[SM] + [HBM] * 4,
        out_specs=[VM] * 5,
        out_shape=[
            pltpu.VMEM((both + TAIL, rows), f32),
            pltpu.VMEM((rows, width), jnp.bfloat16),
            pltpu.VMEM((1, width), f32),
            pltpu.VMEM((HIST, width), f32),
            pltpu.VMEM((HIST, width), f32),
        ],
        scratch_shapes=[
            pltpu.VMEM((rows + LANES, LANES), f32),
            pltpu.VMEM((LANES, width), jnp.bfloat16),
            pltpu.SemaphoreType.DMA((3 + sum(blocks),)),
        ],
        compiler_params=SMALL_GRANT,
        name="load_and_project",
    )(
        lax.axis_index("rows").reshape(1),
        *(pltpu.with_memory_space_constraint(v, pltpu.HBM) for v in (samples, w_row, hist_s, hist_y)),
    )

    bit = 1
    cols = lax.axis_size("cols")
    while 2 * bit < cols:
        pay = pay + hop(pay, "cols", bit)
        bit *= 2
    got = hop(pay, "cols", bit) if cols > 1 else jnp.zeros_like(pay)

    part, gram = pl.pallas_call(
        lambda *refs: second_kernel(chunks, *refs),
        in_specs=[VM] * 4,
        out_specs=[VM] * 2,
        out_shape=[pltpu.VMEM((1, width + LANES), f32), pltpu.VMEM((TAIL, rows), f32)],
        compiler_params=SMALL_GRANT,
        name="residual_and_gradient",
    )(x_in, pay, got, labels.reshape(1, rows))

    coefs = pl.pallas_call(
        solve_kernel,
        in_specs=[SM, VM],
        out_specs=VM,
        out_shape=pltpu.VMEM((both + TAIL, LANES), f32),
        compiler_params=SMALL_GRANT,
        name="solve_history",
    )(counter, gram)

    size = lax.axis_size("rows")
    bit = size // 2
    while bit > 2:
        part = part + hop(part, "rows", bit)
        bit //= 2
    parts = [part] + [hop(part, "rows", k) for k in range(1, min(size, 4))]

    new_w, grad = pl.pallas_call(
        lambda *refs: last_kernel(chunks, len(parts), *refs),
        in_specs=[VM] * (len(parts) + 4),
        out_specs=[VM] * 2,
        out_shape=[jax.ShapeDtypeStruct((1, width), f32)] * 2,
        compiler_params=SMALL_GRANT,
        name="direction_and_update",
    )(*parts, coefs, w_in, s_in, y_in)
    return new_w.reshape(width), grad.reshape(width)


def solution(mesh):
    in_specs = (P("rows", "cols"), P("rows"), P("cols"), P(None, "cols"), P(None, "cols"), P())
    out_specs = (P("cols"), P("cols"))
    return jax.shard_map(body, mesh=mesh, in_specs=in_specs, out_specs=out_specs, check_vma=False)
```

```python
import jax
import jax.numpy as jnp
from jax import lax
from jax.experimental import pallas as pl
from jax.experimental.pallas import tpu as pltpu
from jax.sharding import PartitionSpec as P

HIST = 16
LANES = 128
FOLD = 4
SPOT = 64

penalty = 4.0
step_length = 0.5
highest = lax.Precision.HIGHEST

HBM = pl.BlockSpec(memory_space=pltpu.HBM)
VM = pl.BlockSpec(memory_space=pltpu.VMEM)
SM = pl.BlockSpec(memory_space=pltpu.SMEM)
SMALL_GRANT = pltpu.CompilerParams(vmem_limit_bytes=16 << 20)


def pieces(values):
    out = []
    for _ in range(3):
        part = values.astype(jnp.bfloat16)
        out.append(part)
        values = values - part.astype(jnp.float32)
    return out


def contract_last(left, right):
    dims = (((1,), (1,)), ((), ()))
    return lax.dot_general(left, right, dims, preferred_element_type=jnp.float32)


def first_kernel(blocks, place_ref, x_hbm, w_hbm, s_hbm, y_hbm, pay, x_out, w_out, s_out, y_out, acc, z_buf, sem):
    rows, width = x_out.shape
    both = 2 * HIST
    step = width // sum(blocks)
    smalls = [
        pltpu.make_async_copy(src, dst, sem.at[k])
        for k, (src, dst) in enumerate(((w_hbm, w_out), (s_hbm, s_out), (y_hbm, y_out)))
    ]
    bigs = [
        pltpu.make_async_copy(
            x_hbm.at[:, pl.ds(c * step, step)], x_out.at[:, pl.ds(c * step, step)], sem.at[3 + c]
        )
        for c in range(sum(blocks))
    ]
    for copy in smalls + bigs:
        copy.start()
    live = place_ref[0] >= 0
    for copy in smalls:
        copy.wait()

    @pl.when(live)
    def _():
        part_width = width // 8
        for c in range(8):
            cut = pl.ds(c * part_width, part_width)
            hist = jnp.concatenate([s_out[:, cut], y_out[:, cut]], axis=0)
            for k, part in enumerate(pieces(hist)):
                z_buf[both * k : both * (k + 1), cut] = part
            place = lax.broadcasted_iota(jnp.int32, (both, part_width), 0)
            w_rows = jnp.zeros((both, part_width), jnp.float32)
            for k, part in enumerate(pieces(w_out[:, cut])):
                w_rows = jnp.where(place == k, part.astype(jnp.float32), w_rows)
            z_buf[3 * both :, cut] = w_rows.astype(jnp.bfloat16)
        acc[rows:] = contract_last(z_buf[...], z_buf[...])

    at = 0
    for n, size in enumerate(blocks):
        for c in range(at, at + size):
            bigs[c].wait()

        @pl.when(live)
        def _(n=n, size=size, at=at):
            cut = pl.ds(at * step, size * step)
            product = contract_last(x_out[:, cut], z_buf[:, cut])
            if n == 0:
                acc[:rows] = product
            else:
                acc[:rows] += product

        at += size

    @pl.when(live)
    def _():
        with_x = jnp.transpose(acc[:rows])
        cross = with_x[:both] + (with_x[both : 2 * both] + with_x[2 * both : 3 * both])
        for k in range(both // FOLD):
            pay[k] = cross[FOLD * k : FOLD * (k + 1)]
        with_z = acc[rows:]
        gram = with_z[:both] + (with_z[both : 2 * both] + with_z[2 * both : 3 * both])
        of_y = gram[:, HIST:both] + (gram[:, 3 * HIST : 4 * HIST] + gram[:, 5 * HIST : 6 * HIST])
        at = 6 * HIST
        of_w = gram[:, at : at + 1] + (gram[:, at + 1 : at + 2] + gram[:, at + 2 : at + 3])
        blank = jnp.zeros((HIST, SPOT - both - 2), jnp.float32)
        wide = jnp.concatenate([of_y[:HIST], of_y[HIST:], of_w[:HIST], of_w[HIST:], blank], axis=1)
        wide = jnp.concatenate([wide, jnp.zeros((2, SPOT), jnp.float32)], axis=0)
        laid = jnp.concatenate([wide[3 * k : 3 * k + 3] for k in range(6)], axis=1)
        last = both // FOLD
        pay[last] = jnp.zeros((FOLD, rows), jnp.float32)
        pay[last, :1] = with_x[3 * both : 3 * both + 1]
        pay[last, 1:, : 6 * SPOT] = laid


def second_kernel(chunks, x_ref, own, got, label_ref, pay, gram):
    both = 2 * HIST
    rows, width = x_ref.shape
    step = width // chunks
    last = both // FOLD
    tail = own[last] + got[last]
    gram[...] = tail
    margin = tail[0:1, :]
    resid = (jax.nn.sigmoid(margin) - label_ref[...].astype(jnp.float32)).astype(jnp.bfloat16)
    for c in range(chunks):
        cut = pl.ds(c * step, step)
        pay[:, cut] = jnp.dot(resid, x_ref[:, cut], preferred_element_type=jnp.float32)
    products = jnp.concatenate([own[k] + got[k] for k in range(last)], axis=0)
    cross = products * resid.astype(jnp.float32)
    column = jnp.sum(cross, axis=1, keepdims=True)
    row_at = lax.broadcasted_iota(jnp.int32, (both, LANES), 0)
    lane_at = lax.broadcasted_iota(jnp.int32, (both, LANES), 1)
    pay[:, width:] = jnp.sum(jnp.where(row_at == lane_at, column, 0.0), axis=0, keepdims=True)


def solve_kernel(counter, gram, out):
    newest = lax.rem(counter[0], HIST)
    wide = jnp.concatenate(
        [gram[1:, SPOT * k : SPOT * (k + 1)] for k in range(6)], axis=0
    )[:HIST]
    sy = wide[:, :HIST]
    yy = wide[:, HIST : 2 * HIST]
    row_at = lax.broadcasted_iota(jnp.int32, (HIST, HIST), 0)
    lane_at = lax.broadcasted_iota(jnp.int32, (HIST, HIST), 1)
    row_age = lax.rem(newest - row_at + HIST, HIST)
    lane_age = lax.rem(newest - lane_at + HIST, HIST)
    eye = row_at == lane_at
    diag_col = jnp.sum(jnp.where(eye, sy, 0.0), axis=1, keepdims=True)
    rho_col = 1.0 / diag_col
    strict = jnp.where(lane_age < row_age, sy, 0.0) * rho_col
    rest = jnp.where(eye, rho_col, 0.0)
    for age in range(HIST - 1):
        column = jnp.sum(jnp.where(lane_age == age, strict, 0.0), axis=1, keepdims=True)
        row = jnp.sum(jnp.where(row_age == age, rest, 0.0), axis=0, keepdims=True)
        rest = rest - column * row
    at_new = jnp.logical_and(row_at == newest, lane_at == newest)
    top = jnp.sum(jnp.sum(jnp.where(at_new, sy, 0.0), axis=1, keepdims=True), axis=0, keepdims=True)
    low = jnp.sum(jnp.sum(jnp.where(at_new, yy, 0.0), axis=1, keepdims=True), axis=0, keepdims=True)
    gamma = top / low
    middle = jnp.where(eye, diag_col, 0.0) + gamma * yy
    right = jnp.dot(middle, rest, precision=highest, preferred_element_type=jnp.float32)
    flip = (((0,), (0,)), ((), ()))
    corner = lax.dot_general(rest, right, flip, precision=highest, preferred_element_type=jnp.float32)
    turned = lax.dot_general(
        rest, jnp.where(eye, 1.0, 0.0), flip, precision=highest, preferred_element_type=jnp.float32
    )
    out[...] = jnp.zeros(out.shape, jnp.float32)
    out[0:HIST, 0:HIST] = corner
    out[0:HIST, HIST : 2 * HIST] = -gamma * turned
    out[HIST : 2 * HIST, 0:HIST] = -gamma * rest
    ones = jnp.ones((1, LANES), jnp.float32)
    out[2 * HIST : 2 * HIST + 1, :] = gamma * ones
    w_col = jnp.concatenate([wide[:, 2 * HIST : 2 * HIST + 1], wide[:, 2 * HIST + 1 : 2 * HIST + 2]], axis=0)
    big_row = lax.broadcasted_iota(jnp.int32, (2 * HIST, LANES), 0)
    big_lane = lax.broadcasted_iota(jnp.int32, (2 * HIST, LANES), 1)
    out[2 * HIST + 1 : 2 * HIST + 2, :] = jnp.sum(
        jnp.where(big_row == big_lane, w_col, 0.0), axis=0, keepdims=True
    )


def last_kernel(chunks, count, *refs):
    parts = refs[:count]
    coef_ref, w_ref, s_ref, y_ref, new_ref, grad_ref = refs[count:]
    both = 2 * HIST
    width = w_ref.shape[1]
    step = width // chunks

    def summed(cut):
        level = [p[:, cut] for p in parts]
        while len(level) > 1:
            level = [level[k] + level[k + 1] for k in range(0, len(level), 2)]
        return level[0]

    dots = coef_ref[both + 1 : both + 2, :] + penalty * summed(pl.ds(width, LANES))
    gamma = coef_ref[both : both + 1, 0:1]
    coef = jnp.sum(coef_ref[:both, :] * dots, axis=1, keepdims=True)
    for c in range(chunks):
        cut = pl.ds(c * step, step)
        weights = w_ref[:, cut]
        gradient = weights + penalty * summed(cut)
        grad_ref[:, cut] = gradient
        mixed = coef[:HIST] * s_ref[:, cut] + coef[HIST:] * y_ref[:, cut]
        turn = gamma * gradient + jnp.sum(mixed, axis=0, keepdims=True)
        new_ref[:, cut] = weights - step_length * turn


def hop(values, axis, bit):
    size = lax.axis_size(axis)
    return lax.ppermute(values, axis, [(k, k ^ bit) for k in range(size)])


def body(samples, labels, weights, hist_s, hist_y, counter):
    rows, width = samples.shape
    both = 2 * HIST
    f32 = jnp.float32
    chunks = 8
    blocks = (3, 4, 5, 4)
    w_row = weights.reshape(1, width)
    pay, x_in, w_in, s_in, y_in = pl.pallas_call(
        lambda *refs: first_kernel(blocks, *refs),
        in_specs=[SM] + [HBM] * 4,
        out_specs=[VM] * 5,
        out_shape=[
            pltpu.VMEM((both // FOLD + 1, FOLD, rows), f32),
            pltpu.VMEM((rows, width), jnp.bfloat16),
            pltpu.VMEM((1, width), f32),
            pltpu.VMEM((HIST, width), f32),
            pltpu.VMEM((HIST, width), f32),
        ],
        scratch_shapes=[
            pltpu.VMEM((rows + LANES, LANES), f32),
            pltpu.VMEM((LANES, width), jnp.bfloat16),
            pltpu.SemaphoreType.DMA((3 + sum(blocks),)),
        ],
        compiler_params=SMALL_GRANT,
        name="load_and_project",
    )(
        lax.axis_index("rows").reshape(1),
        *(pltpu.with_memory_space_constraint(v, pltpu.HBM) for v in (samples, w_row, hist_s, hist_y)),
    )

    bit = 1
    cols = lax.axis_size("cols")
    while 2 * bit < cols:
        pay = pay + hop(pay, "cols", bit)
        bit *= 2
    got = hop(pay, "cols", bit) if cols > 1 else jnp.zeros_like(pay)

    part, gram = pl.pallas_call(
        lambda *refs: second_kernel(chunks, *refs),
        in_specs=[VM] * 4,
        out_specs=[VM] * 2,
        out_shape=[pltpu.VMEM((1, width + LANES), f32), pltpu.VMEM((FOLD, rows), f32)],
        compiler_params=SMALL_GRANT,
        name="residual_and_gradient",
    )(x_in, pay, got, labels.reshape(1, rows))

    coefs = pl.pallas_call(
        solve_kernel,
        in_specs=[SM, VM],
        out_specs=VM,
        out_shape=pltpu.VMEM((both + 8, LANES), f32),
        compiler_params=SMALL_GRANT,
        name="solve_history",
    )(counter, gram)

    size = lax.axis_size("rows")
    bit = size // 2
    while bit > 2:
        part = part + hop(part, "rows", bit)
        bit //= 2
    parts = [part] + [hop(part, "rows", k) for k in range(1, min(size, 4))]

    new_w, grad = pl.pallas_call(
        lambda *refs: last_kernel(chunks, len(parts), *refs),
        in_specs=[VM] * (len(parts) + 4),
        out_specs=[VM] * 2,
        out_shape=[jax.ShapeDtypeStruct((1, width), f32)] * 2,
        compiler_params=SMALL_GRANT,
        name="direction_and_update",
    )(*parts, coefs, w_in, s_in, y_in)
    return new_w.reshape(width), grad.reshape(width)


def solution(mesh):
    in_specs = (P("rows", "cols"), P("rows"), P("cols"), P(None, "cols"), P(None, "cols"), P())
    out_specs = (P("cols"), P("cols"))
    return jax.shard_map(body, mesh=mesh, in_specs=in_specs, out_specs=out_specs, check_vma=False)
```

```python
import jax
import jax.numpy as jnp
from jax import lax
from jax.experimental import pallas as pl
from jax.experimental.pallas import tpu as pltpu
from jax.sharding import PartitionSpec as P


HIST = 16
LANES = 128
FOLD = 4
SPOT = 64

penalty = 4.0
step_length = 0.5
highest = lax.Precision.HIGHEST

HBM = pl.BlockSpec(memory_space=pltpu.HBM)
VM = pl.BlockSpec(memory_space=pltpu.VMEM)
SM = pl.BlockSpec(memory_space=pltpu.SMEM)
SMALL_GRANT = pltpu.CompilerParams(vmem_limit_bytes=16 << 20)


def pieces(values):
    out = []
    for _ in range(3):
        part = values.astype(jnp.bfloat16)
        out.append(part)
        values = values - part.astype(jnp.float32)
    return out


def contract_last(left, right):
    dims = (((1,), (1,)), ((), ()))
    return lax.dot_general(left, right, dims, preferred_element_type=jnp.float32)


def first_kernel(blocks, place_ref, x_hbm, w_hbm, s_hbm, y_hbm, pay, x_out, w_out, s_out, y_out, acc, z_buf, sem):
    rows, width = x_out.shape
    both = 2 * HIST
    step = width // sum(blocks)
    smalls = [
        pltpu.make_async_copy(src, dst, sem.at[k])
        for k, (src, dst) in enumerate(((w_hbm, w_out), (s_hbm, s_out), (y_hbm, y_out)))
    ]
    bigs = [
        pltpu.make_async_copy(
            x_hbm.at[:, pl.ds(c * step, step)], x_out.at[:, pl.ds(c * step, step)], sem.at[3 + c]
        )
        for c in range(sum(blocks))
    ]
    for copy in smalls + bigs:
        copy.start()
    live = place_ref[0] >= 0
    for copy in smalls:
        copy.wait()

    @pl.when(live)
    def _():
        part_width = width // 8
        for c in range(8):
            cut = pl.ds(c * part_width, part_width)
            hist = jnp.concatenate([s_out[:, cut], y_out[:, cut]], axis=0)
            for k, part in enumerate(pieces(hist)):
                z_buf[both * k : both * (k + 1), cut] = part
            place = lax.broadcasted_iota(jnp.int32, (both, part_width), 0)
            w_rows = jnp.zeros((both, part_width), jnp.float32)
            for k, part in enumerate(pieces(w_out[:, cut])):
                w_rows = jnp.where(place == k, part.astype(jnp.float32), w_rows)
            z_buf[3 * both :, cut] = w_rows.astype(jnp.bfloat16)
        acc[rows:] = contract_last(z_buf[...], z_buf[...])

    at = 0
    for n, size in enumerate(blocks):
        for c in range(at, at + size):
            bigs[c].wait()

        @pl.when(live)
        def _(n=n, size=size, at=at):
            cut = pl.ds(at * step, size * step)
            product = contract_last(x_out[:, cut], z_buf[:, cut])
            if n == 0:
                acc[:rows] = product
            else:
                acc[:rows] += product

        at += size

    @pl.when(live)
    def _():
        with_x = jnp.transpose(acc[:rows])
        cross = with_x[:both] + (with_x[both : 2 * both] + with_x[2 * both : 3 * both])
        for k in range(both // FOLD):
            pay[k] = cross[FOLD * k : FOLD * (k + 1)]
        with_z = acc[rows:]
        gram = with_z[:both] + (with_z[both : 2 * both] + with_z[2 * both : 3 * both])
        of_y = gram[:, HIST:both] + (gram[:, 3 * HIST : 4 * HIST] + gram[:, 5 * HIST : 6 * HIST])
        at = 6 * HIST
        of_w = gram[:, at : at + 1] + (gram[:, at + 1 : at + 2] + gram[:, at + 2 : at + 3])
        blank = jnp.zeros((HIST, SPOT - both - 2), jnp.float32)
        wide = jnp.concatenate([of_y[:HIST], of_y[HIST:], of_w[:HIST], of_w[HIST:], blank], axis=1)
        wide = jnp.concatenate([wide, jnp.zeros((2, SPOT), jnp.float32)], axis=0)
        laid = jnp.concatenate([wide[3 * k : 3 * k + 3] for k in range(6)], axis=1)
        last = both // FOLD
        pay[last] = jnp.zeros((FOLD, rows), jnp.float32)
        pay[last, :1] = with_x[3 * both : 3 * both + 1]
        pay[last, 1:, : 6 * SPOT] = laid


def second_kernel(chunks, x_ref, own, got, label_ref, pay, gram):
    both = 2 * HIST
    _, width = x_ref.shape
    step = width // chunks
    last = both // FOLD
    tail = own[last] + got[last]
    gram[...] = tail
    margin = tail[0:1, :]
    resid = (jax.nn.sigmoid(margin) - label_ref[...].astype(jnp.float32)).astype(jnp.bfloat16)
    for c in range(chunks):
        cut = pl.ds(c * step, step)
        pay[:, cut] = jnp.dot(resid, x_ref[:, cut], preferred_element_type=jnp.float32)
    products = jnp.concatenate([own[k] + got[k] for k in range(last)], axis=0)
    cross = products * resid.astype(jnp.float32)
    column = jnp.sum(cross, axis=1, keepdims=True)
    row_at = lax.broadcasted_iota(jnp.int32, (both, LANES), 0)
    lane_at = lax.broadcasted_iota(jnp.int32, (both, LANES), 1)
    pay[:, width:] = jnp.sum(jnp.where(row_at == lane_at, column, 0.0), axis=0, keepdims=True)


def solve_kernel(counter, gram, out):
    newest = lax.rem(counter[0], HIST)
    wide = jnp.concatenate(
        [gram[1:, SPOT * k : SPOT * (k + 1)] for k in range(6)], axis=0
    )[:HIST]
    sy = wide[:, :HIST]
    yy = wide[:, HIST : 2 * HIST]
    row_at = lax.broadcasted_iota(jnp.int32, (HIST, HIST), 0)
    lane_at = lax.broadcasted_iota(jnp.int32, (HIST, HIST), 1)
    row_age = lax.rem(newest - row_at + HIST, HIST)
    lane_age = lax.rem(newest - lane_at + HIST, HIST)
    eye = row_at == lane_at
    diag_col = jnp.sum(jnp.where(eye, sy, 0.0), axis=1, keepdims=True)
    rho_col = 1.0 / diag_col
    strict = jnp.where(lane_age < row_age, sy, 0.0) * rho_col
    rest = jnp.where(eye, rho_col, 0.0)
    for age in range(HIST - 1):
        column = jnp.sum(jnp.where(lane_age == age, strict, 0.0), axis=1, keepdims=True)
        row = jnp.sum(jnp.where(row_age == age, rest, 0.0), axis=0, keepdims=True)
        rest = rest - column * row
    at_new = jnp.logical_and(row_at == newest, lane_at == newest)
    top = jnp.sum(jnp.sum(jnp.where(at_new, sy, 0.0), axis=1, keepdims=True), axis=0, keepdims=True)
    low = jnp.sum(jnp.sum(jnp.where(at_new, yy, 0.0), axis=1, keepdims=True), axis=0, keepdims=True)
    gamma = top / low
    middle = jnp.where(eye, diag_col, 0.0) + gamma * yy
    right = jnp.dot(middle, rest, precision=highest, preferred_element_type=jnp.float32)
    flip = (((0,), (0,)), ((), ()))
    corner = lax.dot_general(rest, right, flip, precision=highest, preferred_element_type=jnp.float32)
    turned = lax.dot_general(
        rest, jnp.where(eye, 1.0, 0.0), flip, precision=highest, preferred_element_type=jnp.float32
    )
    out[...] = jnp.zeros(out.shape, jnp.float32)
    out[0:HIST, 0:HIST] = corner
    out[0:HIST, HIST : 2 * HIST] = -gamma * turned
    out[HIST : 2 * HIST, 0:HIST] = -gamma * rest
    ones = jnp.ones((1, LANES), jnp.float32)
    out[2 * HIST : 2 * HIST + 1, :] = gamma * ones
    w_col = jnp.concatenate([wide[:, 2 * HIST : 2 * HIST + 1], wide[:, 2 * HIST + 1 : 2 * HIST + 2]], axis=0)
    big_row = lax.broadcasted_iota(jnp.int32, (2 * HIST, LANES), 0)
    big_lane = lax.broadcasted_iota(jnp.int32, (2 * HIST, LANES), 1)
    out[2 * HIST + 1 : 2 * HIST + 2, :] = jnp.sum(
        jnp.where(big_row == big_lane, w_col, 0.0), axis=0, keepdims=True
    )


def last_kernel(chunks, count, *refs):
    parts = refs[:count]
    coef_ref, w_ref, s_ref, y_ref, new_ref, grad_ref = refs[count:]
    both = 2 * HIST
    width = w_ref.shape[1]
    step = width // chunks

    def summed(cut):
        level = [p[:, cut] for p in parts]
        while len(level) > 1:
            level = [level[k] + level[k + 1] for k in range(0, len(level), 2)]
        return level[0]

    dots = coef_ref[both + 1 : both + 2, :] + penalty * summed(pl.ds(width, LANES))
    gamma = coef_ref[both : both + 1, 0:1]
    coef = jnp.sum(coef_ref[:both, :] * dots, axis=1, keepdims=True)
    for c in range(chunks):
        cut = pl.ds(c * step, step)
        weights = w_ref[:, cut]
        gradient = weights + penalty * summed(cut)
        grad_ref[:, cut] = gradient
        mixed = coef[:HIST] * s_ref[:, cut] + coef[HIST:] * y_ref[:, cut]
        turn = gamma * gradient + jnp.sum(mixed, axis=0, keepdims=True)
        new_ref[:, cut] = weights - step_length * turn


def hop(values, axis, bit):
    size = lax.axis_size(axis)
    return lax.ppermute(values, axis, [(k, k ^ bit) for k in range(size)])


def body(samples, labels, weights, hist_s, hist_y, counter):
    rows, width = samples.shape
    both = 2 * HIST
    f32 = jnp.float32
    chunks = 8
    blocks = (3, 4, 5, 4)
    w_row = weights.reshape(1, width)
    pay, x_in, w_in, s_in, y_in = pl.pallas_call(
        lambda *refs: first_kernel(blocks, *refs),
        in_specs=[SM] + [HBM] * 4,
        out_specs=[VM] * 5,
        out_shape=[
            pltpu.VMEM((both // FOLD + 1, FOLD, rows), f32),
            pltpu.VMEM((rows, width), jnp.bfloat16),
            pltpu.VMEM((1, width), f32),
            pltpu.VMEM((HIST, width), f32),
            pltpu.VMEM((HIST, width), f32),
        ],
        scratch_shapes=[
            pltpu.VMEM((rows + LANES, LANES), f32),
            pltpu.VMEM((LANES, width), jnp.bfloat16),
            pltpu.SemaphoreType.DMA((3 + sum(blocks),)),
        ],
        compiler_params=SMALL_GRANT,
        name="load_and_project",
    )(
        lax.axis_index("rows").reshape(1),
        *(pltpu.with_memory_space_constraint(v, pltpu.HBM) for v in (samples, w_row, hist_s, hist_y)),
    )

    cols = lax.axis_size("cols")
    bit = cols // 2
    while bit > 2:
        pay = pay + hop(pay, "cols", bit)
        bit //= 2
    near = {k: hop(pay, "cols", k) for k in (1, 2, 3) if k < cols}
    if cols >= 4:
        own, got = pay + near[1], near[2] + near[3]
    else:
        own, got = pay, near[1] if cols > 1 else jnp.zeros_like(pay)

    part, gram = pl.pallas_call(
        lambda *refs: second_kernel(chunks, *refs),
        in_specs=[VM] * 4,
        out_specs=[VM] * 2,
        out_shape=[pltpu.VMEM((1, width + LANES), f32), pltpu.VMEM((FOLD, rows), f32)],
        compiler_params=SMALL_GRANT,
        name="residual_and_gradient",
    )(x_in, own, got, labels.reshape(1, rows))

    coefs = pl.pallas_call(
        solve_kernel,
        in_specs=[SM, VM],
        out_specs=VM,
        out_shape=pltpu.VMEM((both + 8, LANES), f32),
        compiler_params=SMALL_GRANT,
        name="solve_history",
    )(counter, gram)

    size = lax.axis_size("rows")
    bit = size // 2
    while bit > 2:
        part = part + hop(part, "rows", bit)
        bit //= 2
    parts = [part] + [hop(part, "rows", k) for k in range(1, min(size, 4))]

    new_w, grad = pl.pallas_call(
        lambda *refs: last_kernel(chunks, len(parts), *refs),
        in_specs=[VM] * (len(parts) + 4),
        out_specs=[VM] * 2,
        out_shape=[jax.ShapeDtypeStruct((1, width), f32)] * 2,
        compiler_params=SMALL_GRANT,
        name="direction_and_update",
    )(*parts, coefs, w_in, s_in, y_in)
    return new_w.reshape(width), grad.reshape(width)


def solution(mesh):
    in_specs = (P("rows", "cols"), P("rows"), P("cols"), P(None, "cols"), P(None, "cols"), P())
    out_specs = (P("cols"), P("cols"))

    return jax.shard_map(body, mesh=mesh, in_specs=in_specs, out_specs=out_specs, check_vma=False)
```

```python
import jax
import jax.numpy as jnp
from jax import lax
from jax.experimental import pallas as pl
from jax.experimental.pallas import tpu as pltpu
from jax.sharding import PartitionSpec as P


HIST = 16
LANES = 128
FOLD = 4
SPOT = 64

penalty = 4.0
step_length = 0.5
highest = lax.Precision.HIGHEST

HBM = pl.BlockSpec(memory_space=pltpu.HBM)
VM = pl.BlockSpec(memory_space=pltpu.VMEM)
SM = pl.BlockSpec(memory_space=pltpu.SMEM)
SMALL_GRANT = pltpu.CompilerParams(vmem_limit_bytes=16 << 20)


def pieces(values):
    out = []
    for _ in range(3):
        part = values.astype(jnp.bfloat16)
        out.append(part)
        values = values - part.astype(jnp.float32)
    return out


def contract_last(left, right):
    dims = (((1,), (1,)), ((), ()))
    return lax.dot_general(left, right, dims, preferred_element_type=jnp.float32)


def first_kernel(blocks, place_ref, x_hbm, w_hbm, s_hbm, y_hbm, pay, x_out, w_out, s_out, y_out, acc, z_buf, sem):
    rows, width = x_out.shape
    both = 2 * HIST
    step = width // sum(blocks)
    smalls = [
        pltpu.make_async_copy(src, dst, sem.at[k])
        for k, (src, dst) in enumerate(((w_hbm, w_out), (s_hbm, s_out), (y_hbm, y_out)))
    ]
    bigs = [
        pltpu.make_async_copy(
            x_hbm.at[:, pl.ds(c * step, step)], x_out.at[:, pl.ds(c * step, step)], sem.at[3 + c]
        )
        for c in range(sum(blocks))
    ]
    for copy in smalls + bigs:
        copy.start()
    live = place_ref[0] >= 0
    for copy in smalls:
        copy.wait()

    @pl.when(live)
    def _():
        part_width = width // 8
        for c in range(8):
            cut = pl.ds(c * part_width, part_width)
            hist = jnp.concatenate([s_out[:, cut], y_out[:, cut]], axis=0)
            for k, part in enumerate(pieces(hist)):
                z_buf[both * k : both * (k + 1), cut] = part
            place = lax.broadcasted_iota(jnp.int32, (both, part_width), 0)
            w_rows = jnp.zeros((both, part_width), jnp.float32)
            for k, part in enumerate(pieces(w_out[:, cut])):
                w_rows = jnp.where(place == k, part.astype(jnp.float32), w_rows)
            z_buf[3 * both :, cut] = w_rows.astype(jnp.bfloat16)
        acc[rows:] = contract_last(z_buf[...], z_buf[...])

    at = 0
    for n, size in enumerate(blocks):
        for c in range(at, at + size):
            bigs[c].wait()

        @pl.when(live)
        def _(n=n, size=size, at=at):
            cut = pl.ds(at * step, size * step)
            product = contract_last(x_out[:, cut], z_buf[:, cut])
            if n == 0:
                acc[:rows] = product
            else:
                acc[:rows] += product

        at += size

    @pl.when(live)
    def _():
        with_x = jnp.transpose(acc[:rows])
        cross = with_x[:both] + (with_x[both : 2 * both] + with_x[2 * both : 3 * both])
        for k in range(both // FOLD):
            pay[k] = cross[FOLD * k : FOLD * (k + 1)]
        with_z = acc[rows:]
        gram = with_z[:both] + (with_z[both : 2 * both] + with_z[2 * both : 3 * both])
        of_y = gram[:, HIST:both] + (gram[:, 3 * HIST : 4 * HIST] + gram[:, 5 * HIST : 6 * HIST])
        at = 6 * HIST
        of_w = gram[:, at : at + 1] + (gram[:, at + 1 : at + 2] + gram[:, at + 2 : at + 3])
        blank = jnp.zeros((HIST, SPOT - both - 2), jnp.float32)
        wide = jnp.concatenate([of_y[:HIST], of_y[HIST:], of_w[:HIST], of_w[HIST:], blank], axis=1)
        wide = jnp.concatenate([wide, jnp.zeros((2, SPOT), jnp.float32)], axis=0)
        laid = jnp.concatenate([wide[3 * k : 3 * k + 3] for k in range(6)], axis=1)
        last = both // FOLD
        pay[last] = jnp.zeros((FOLD, rows), jnp.float32)
        pay[last, :1] = with_x[3 * both : 3 * both + 1]
        pay[last, 1:, : 6 * SPOT] = laid


def second_kernel(chunks, x_ref, own, got, label_ref, pay, gram):
    both = 2 * HIST
    _, width = x_ref.shape
    step = width // chunks
    last = both // FOLD
    tail = own[last] + got[last]
    gram[...] = tail
    margin = tail[0:1, :]
    resid = (jax.nn.sigmoid(margin) - label_ref[...].astype(jnp.float32)).astype(jnp.bfloat16)
    for c in range(chunks):
        cut = pl.ds(c * step, step)
        pay[:, cut] = jnp.dot(resid, x_ref[:, cut], preferred_element_type=jnp.float32)
    products = jnp.concatenate([own[k] + got[k] for k in range(last)], axis=0)
    cross = products * resid.astype(jnp.float32)
    column = jnp.sum(cross, axis=1, keepdims=True)
    row_at = lax.broadcasted_iota(jnp.int32, (both, LANES), 0)
    lane_at = lax.broadcasted_iota(jnp.int32, (both, LANES), 1)
    pay[:, width:] = jnp.sum(jnp.where(row_at == lane_at, column, 0.0), axis=0, keepdims=True)


def solve_kernel(counter, gram, out):
    newest = lax.rem(counter[0], HIST)
    wide = jnp.concatenate(
        [gram[1:, SPOT * k : SPOT * (k + 1)] for k in range(6)], axis=0
    )[:HIST]
    sy = wide[:, :HIST]
    yy = wide[:, HIST : 2 * HIST]
    row_at = lax.broadcasted_iota(jnp.int32, (HIST, HIST), 0)
    lane_at = lax.broadcasted_iota(jnp.int32, (HIST, HIST), 1)
    row_age = lax.rem(newest - row_at + HIST, HIST)
    lane_age = lax.rem(newest - lane_at + HIST, HIST)
    eye = row_at == lane_at
    diag_col = jnp.sum(jnp.where(eye, sy, 0.0), axis=1, keepdims=True)
    rho_col = 1.0 / diag_col
    strict = jnp.where(lane_age < row_age, sy, 0.0) * rho_col
    rest = jnp.where(eye, rho_col, 0.0)
    for age in range(HIST - 1):
        column = jnp.sum(jnp.where(lane_age == age, strict, 0.0), axis=1, keepdims=True)
        row = jnp.sum(jnp.where(row_age == age, rest, 0.0), axis=0, keepdims=True)
        rest = rest - column * row
    at_new = jnp.logical_and(row_at == newest, lane_at == newest)
    top = jnp.sum(jnp.sum(jnp.where(at_new, sy, 0.0), axis=1, keepdims=True), axis=0, keepdims=True)
    low = jnp.sum(jnp.sum(jnp.where(at_new, yy, 0.0), axis=1, keepdims=True), axis=0, keepdims=True)
    gamma = top / low
    middle = jnp.where(eye, diag_col, 0.0) + gamma * yy
    right = jnp.dot(middle, rest, precision=highest, preferred_element_type=jnp.float32)
    flip = (((0,), (0,)), ((), ()))
    corner = lax.dot_general(rest, right, flip, precision=highest, preferred_element_type=jnp.float32)
    turned = lax.dot_general(
        rest, jnp.where(eye, 1.0, 0.0), flip, precision=highest, preferred_element_type=jnp.float32
    )
    out[...] = jnp.zeros(out.shape, jnp.float32)
    out[0:HIST, 0:HIST] = corner
    out[0:HIST, HIST : 2 * HIST] = -gamma * turned
    out[HIST : 2 * HIST, 0:HIST] = -gamma * rest
    ones = jnp.ones((1, LANES), jnp.float32)
    out[2 * HIST : 2 * HIST + 1, :] = gamma * ones
    w_col = jnp.concatenate([wide[:, 2 * HIST : 2 * HIST + 1], wide[:, 2 * HIST + 1 : 2 * HIST + 2]], axis=0)
    big_row = lax.broadcasted_iota(jnp.int32, (2 * HIST, LANES), 0)
    big_lane = lax.broadcasted_iota(jnp.int32, (2 * HIST, LANES), 1)
    out[2 * HIST + 1 : 2 * HIST + 2, :] = jnp.sum(
        jnp.where(big_row == big_lane, w_col, 0.0), axis=0, keepdims=True
    )


def last_kernel(chunks, count, *refs):
    parts = refs[:count]
    coef_ref, w_ref, s_ref, y_ref, new_hbm, grad_hbm, new_ref, grad_ref, sem = refs[count:]
    both = 2 * HIST
    width = w_ref.shape[1]
    step = width // chunks

    def summed(cut):
        level = [p[:, cut] for p in parts]
        while len(level) > 1:
            level = [level[k] + level[k + 1] for k in range(0, len(level), 2)]
        return level[0]

    dots = coef_ref[both + 1 : both + 2, :] + penalty * summed(pl.ds(width, LANES))
    gamma = coef_ref[both : both + 1, 0:1]
    coef = jnp.sum(coef_ref[:both, :] * dots, axis=1, keepdims=True)
    for c in range(chunks):
        cut = pl.ds(c * step, step)
        grad_ref[:, cut] = w_ref[:, cut] + penalty * summed(cut)
    copies = [pltpu.make_async_copy(grad_ref, grad_hbm, sem.at[0])]
    copies[0].start()
    for c in range(chunks):
        cut = pl.ds(c * step, step)
        mixed = coef[:HIST] * s_ref[:, cut] + coef[HIST:] * y_ref[:, cut]
        turn = gamma * grad_ref[:, cut] + jnp.sum(mixed, axis=0, keepdims=True)
        new_ref[:, cut] = w_ref[:, cut] - step_length * turn
    copies.append(pltpu.make_async_copy(new_ref, new_hbm, sem.at[1]))
    copies[1].start()
    for copy in copies:
        copy.wait()


def hop(values, axis, bit):
    size = lax.axis_size(axis)
    return lax.ppermute(values, axis, [(k, k ^ bit) for k in range(size)])


def body(samples, labels, weights, hist_s, hist_y, counter):
    rows, width = samples.shape
    both = 2 * HIST
    f32 = jnp.float32
    chunks = 8
    blocks = (3, 4, 5, 4)
    w_row = weights.reshape(1, width)
    pay, x_in, w_in, s_in, y_in = pl.pallas_call(
        lambda *refs: first_kernel(blocks, *refs),
        in_specs=[SM] + [HBM] * 4,
        out_specs=[VM] * 5,
        out_shape=[
            pltpu.VMEM((both // FOLD + 1, FOLD, rows), f32),
            pltpu.VMEM((rows, width), jnp.bfloat16),
            pltpu.VMEM((1, width), f32),
            pltpu.VMEM((HIST, width), f32),
            pltpu.VMEM((HIST, width), f32),
        ],
        scratch_shapes=[
            pltpu.VMEM((rows + LANES, LANES), f32),
            pltpu.VMEM((LANES, width), jnp.bfloat16),
            pltpu.SemaphoreType.DMA((3 + sum(blocks),)),
        ],
        compiler_params=SMALL_GRANT,
        name="load_and_project",
    )(
        lax.axis_index("rows").reshape(1),
        *(pltpu.with_memory_space_constraint(v, pltpu.HBM) for v in (samples, w_row, hist_s, hist_y)),
    )

    cols = lax.axis_size("cols")
    bit = cols // 2
    while bit > 2:
        pay = pay + hop(pay, "cols", bit)
        bit //= 2
    near = {k: hop(pay, "cols", k) for k in (1, 2, 3) if k < cols}
    if cols >= 4:
        own, got = pay + near[1], near[2] + near[3]
    else:
        own, got = pay, near[1] if cols > 1 else jnp.zeros_like(pay)

    part, gram = pl.pallas_call(
        lambda *refs: second_kernel(chunks, *refs),
        in_specs=[VM] * 4,
        out_specs=[VM] * 2,
        out_shape=[pltpu.VMEM((1, width + LANES), f32), pltpu.VMEM((FOLD, rows), f32)],
        compiler_params=SMALL_GRANT,
        name="residual_and_gradient",
    )(x_in, own, got, labels.reshape(1, rows))

    coefs = pl.pallas_call(
        solve_kernel,
        in_specs=[SM, VM],
        out_specs=VM,
        out_shape=pltpu.VMEM((both + 8, LANES), f32),
        compiler_params=SMALL_GRANT,
        name="solve_history",
    )(counter, gram)

    size = lax.axis_size("rows")
    bit = size // 2
    while bit > 2:
        part = part + hop(part, "rows", bit)
        bit //= 2
    parts = [part] + [hop(part, "rows", k) for k in range(1, min(size, 4))]

    new_w, grad = pl.pallas_call(
        lambda *refs: last_kernel(chunks, len(parts), *refs),
        in_specs=[VM] * (len(parts) + 4),
        out_specs=[HBM] * 2,
        out_shape=[jax.ShapeDtypeStruct((1, width), f32)] * 2,
        scratch_shapes=[
            pltpu.VMEM((1, width), f32),
            pltpu.VMEM((1, width), f32),
            pltpu.SemaphoreType.DMA((2,)),
        ],
        compiler_params=SMALL_GRANT,
        name="direction_and_update",
    )(*parts, coefs, w_in, s_in, y_in)
    return new_w.reshape(width), grad.reshape(width)


def solution(mesh):
    in_specs = (P("rows", "cols"), P("rows"), P("cols"), P(None, "cols"), P(None, "cols"), P())
    out_specs = (P("cols"), P("cols"))

    return jax.shard_map(body, mesh=mesh, in_specs=in_specs, out_specs=out_specs, check_vma=False)
```
